256 devices in a mesh: dp: 8 (over x, core), expert: 32 (over y, z).
Axes of the slice: x: 4, y: 4, z: 8, core: 2. Of those that a mesh axis runs over, the one named last changes fastest.
Arguments:
- tokens: bfloat16 [4096, 5120], P('expert', 'dp'), may hold values from -6 to 6
- out_grad: bfloat16 [4096, 5120], P('expert', 'dp'), may hold values from -0.59765625 to 0.59765625
- gate_values: float32 [4096, 8], P('expert'), may hold values from 0.05 to 0.5
- route_lists: int32 [4096, 8], P('expert'), may hold values from 0 to 15, all different within a row; in each aligned block of 128 rows (0 to 127, 128 to 255, ...) at most 72 rows name the same one
- expert_pairs: int32 [16], replicated, may hold values from 0 to 15, as said below
- gate_weight: bfloat16 [32, 5120, 1024], P('expert', 'dp'), as said below
- up_weight: bfloat16 [32, 5120, 1024], P('expert', 'dp'), as said below
- down_weight: bfloat16 [32, 1024, 5120], P('expert', None, 'dp'), as said below
Outputs:
- layer_output: bfloat16 [4096, 5120], P('expert', 'dp')
- token_grad: bfloat16 [4096, 5120], P('expert', 'dp')
- gate_value_grad: float32 [4096, 8], P('expert')
- gate_weight_grad: bfloat16 [32, 5120, 1024], P('expert', 'dp')
- up_weight_grad: bfloat16 [32, 5120, 1024], P('expert', 'dp')
- down_weight_grad: bfloat16 [32, 1024, 5120], P('expert', None, 'dp')
The draws below stay inside these ranges and needn't reach their ends.
Inputs may be any that keep to these rules, and one draw needn't show every extreme that they name: `route_lists`: each token names 8 different experts; within each aligned block of 128 tokens no expert is named by more than 72 tokens. `expert_pairs`: a permutation; pair p is made of slots p and p + 16. `gate_weight`: slots p and p + 16 hold equal matrices, those of expert expert_pairs[p]. `up_weight`: slots p and p + 16 hold equal matrices. `down_weight`: slots p and p + 16 hold equal matrices.
All inputs are finite; a program needn't handle non-finite values.
Results may differ from the reference program's by a relative error of at most 0.023.
Values may be sent and summed in bfloat16 or wider, within the bound.
A program may use at most 128 MiB of HBM per device.

```python
import math
import jax
import jax.numpy as jnp
import numpy as np
from jax import lax

D = 5120
FF = 1024
TOK_DEV = 128
CAP = 72
HALF = 36
EXPERTS = 16
TOP = 8
TOKENS = 4096
N_DP = 8
N_EXPERT = 32


def pairing(key):
    return jax.random.permutation(jax.random.fold_in(key, 4242), EXPERTS).astype(jnp.int32)


def slot_matrices(key, salt, row_size, col_size, scale):
    order = pairing(key)
    slot_experts = order[jnp.arange(2 * EXPERTS, dtype=jnp.int32) % EXPERTS]
    base_key = jax.random.fold_in(key, salt)

    def one_slot(expert_id):
        slot_key = jax.random.fold_in(base_key, expert_id)
        values = jax.random.normal(slot_key, (row_size, col_size), jnp.float32)
        return values * scale
    return jax.vmap(one_slot)(slot_experts)


def draw_expert_pairs(key, part):
    return pairing(key)


def draw_gate_weight(key, part):
    return slot_matrices(key, 11, D, FF, D ** (-0.5)).astype(jnp.bfloat16)


def draw_up_weight(key, part):
    return slot_matrices(key, 12, D, FF, D ** (-0.5)).astype(jnp.bfloat16)


def draw_down_weight(key, part):
    return slot_matrices(key, 13, FF, D, FF ** (-0.5)).astype(jnp.bfloat16)


def steps_of(key, extent, shards, least, top_value):
    gain, own = 1.0, jax.random.fold_in(key, 6)
    for axis_at, parts in shards:
        heights = jnp.exp(jax.random.uniform(jax.random.fold_in(own, axis_at), (parts,), jnp.float32, least / len(shards), top_value / len(shards)))
        gain = gain * jnp.repeat(heights, extent[axis_at] // parts).reshape([-1 if axis == axis_at else 1 for axis in range(len(extent))])
    return gain


def routed_block(key, own, number, rows, number_of, top, reach, slope):
    order = jax.random.permutation(key, number_of)
    crowded, common = portions_of(number_of, rows * top, reach, slope, True), portions_of(number_of, rows * top, reach, slope, False)
    places = jnp.arange(number_of)

    def named(tallies, offset_by):
        used = int((tallies > 0).sum())
        fixed = max(1, used // 4)
        moved = fixed + (places - fixed + offset_by * (used - fixed)) % max(1, number_of - fixed)
        return jnp.zeros((number_of,), jnp.int32).at[order[jnp.where(places < fixed, places, moved)]].set(jnp.asarray(tallies, jnp.int32))

    tallies = jnp.where(number % 4 == 0, named(crowded, number // 4), named(common, number - number // 4 - 1))
    mixed = jax.random.permutation(jax.random.fold_in(own, 3), number_of)
    donor, taker = mixed[0:number_of // 2 * 2:2], mixed[1:number_of // 2 * 2:2]
    margin = jnp.minimum(tallies[donor] - 1, reach - tallies[taker]) // 2
    margin = jnp.where((donor == order[0]) | (taker == order[0]) | (tallies[taker] == 0), 0, jnp.maximum(margin, 0))
    moved = jax.random.randint(jax.random.fold_in(own, 4), (number_of // 2,), 0, 1 << 20) % (margin + 1)
    tallies = tallies.at[donor].add(-moved).at[taker].add(moved)
    labels = jnp.searchsorted(jnp.cumsum(tallies), jnp.arange(rows * top), side="right").astype(jnp.int32)
    grid = labels.reshape(top, rows).T
    grid = grid[jax.random.permutation(jax.random.fold_in(own, 1), rows)]
    offset_by = jax.random.randint(jax.random.fold_in(own, 2), (rows, 1), 0, top)
    return jnp.take_along_axis(grid, (jnp.arange(top)[None, :] + offset_by) % top, axis=1)


def portions_of(number_of, total, limit, slope, full):
    weights = [(1 << 20) // math.isqrt(grade ** slope) + 1 for grade in range(1, number_of + 1)]
    largest = limit if full else min(limit, max(-(-total // number_of), total * weights[0] // sum(weights)))
    least = 1 if total - largest >= number_of - 1 else 0
    holding, surplus = [largest] + [least] * (number_of - 1), total - largest - least * (number_of - 1)
    while surplus > 0:
        free = [i for i in range(1, number_of) if holding[i] < largest] or [i for i in range(1, number_of) if holding[i] < limit]
        whole, left = sum([weights[i] for i in free]), surplus
        for i in free:
            extra = min(limit - holding[i], max(1, left * weights[i] // whole), surplus)
            holding[i] = holding[i] + extra
            surplus = surplus - extra
    return np.array(holding)


def bell_draw(rng, shape, scale, bound, pieces=(), held_as=jnp.bfloat16):
    loudness = steps_of(rng, shape, pieces, -0.22, 0.18) if pieces else 1.0
    values = jax.random.normal(rng, shape, jnp.float32) * scale * loudness
    return jnp.minimum(jnp.maximum(values, -bound), bound).astype(held_as)


def setup_inputs(seed: int = 0) -> dict:
    seeds = jax.random.split(jax.random.key(seed), 9)
    tokens = bell_draw(seeds[0], (TOKENS, D), 1.0, 6.0, ((0, 32), (1, 8)))
    out_grad = bell_draw(seeds[1], (TOKENS, D), 0.1, 0.59765625, ((0, 32), (1, 8)))
    gate_values = jnp.clip(0.05 + 0.45 * jax.random.uniform(seeds[2], (TOKENS, TOP), jnp.float32) ** steps_of(seeds[2], (TOKENS, TOP), ((0, 32),), -0.2, 0.2), 0.05, 0.5)
    route_lists_keys = jax.random.split(jax.random.fold_in(seeds[3], 1), TOKENS // TOK_DEV)
    route_lists_turns = jax.random.permutation(jax.random.fold_in(seeds[3], 3), TOKENS // TOK_DEV)
    route_lists = jax.vmap(lambda own, number: routed_block(jax.random.fold_in(seeds[3], 2), own, number, TOK_DEV, EXPERTS, TOP, CAP, 2))(route_lists_keys, route_lists_turns).reshape((TOKENS, TOP))
    expert_pairs = draw_expert_pairs(jax.random.fold_in(seeds[8], 71), 0)
    gate_weight = draw_gate_weight(jax.random.fold_in(seeds[8], 71), 0)
    up_weight = draw_up_weight(jax.random.fold_in(seeds[8], 71), 0)
    down_weight = draw_down_weight(jax.random.fold_in(seeds[8], 71), 0)
    return {"tokens": tokens, "out_grad": out_grad, "gate_values": gate_values, "route_lists": route_lists, "expert_pairs": expert_pairs, "gate_weight": gate_weight, "up_weight": up_weight, "down_weight": down_weight}


def rounded(values):
    return lax.optimization_barrier(values.astype(jnp.bfloat16)).astype(jnp.float32)


def block_sums(rows_in, weight):
    width_dev = D // N_DP
    row_blocks = rows_in.astype(jnp.float32).reshape(rows_in.shape[0], N_DP, width_dev)
    weight_blocks = weight.astype(jnp.float32).reshape(N_DP, width_dev, weight.shape[1])
    partial_terms = jnp.einsum("rdk,dkf->rdf", row_blocks, weight_blocks)
    return jnp.sum(rounded(partial_terms), axis=1)


def back_block_sums(rows_in, weight):
    width_dev = D // N_DP
    row_blocks = rows_in.astype(jnp.float32).reshape(rows_in.shape[0], N_DP, width_dev)
    weight_blocks = weight.astype(jnp.float32).reshape(weight.shape[0], N_DP, width_dev)
    partial_terms = jnp.einsum("rdk,fdk->rdf", row_blocks, weight_blocks)
    return jnp.sum(rounded(partial_terms), axis=1)


def reference(tokens, out_grad, gate_values, route_lists, expert_pairs, gate_weight, up_weight, down_weight):
    catalog = jnp.arange(EXPERTS, dtype=jnp.int32)
    chosen = route_lists[:, :, None] == catalog[None, None, :]
    present = jnp.sum(chosen.astype(jnp.int32), axis=1)
    blocked = present.reshape(N_EXPERT, TOK_DEV, EXPERTS)
    before = (jnp.cumsum(blocked, axis=1) - blocked).reshape(TOKENS, EXPERTS)
    weight_sel = jnp.sum(jnp.where(chosen, gate_values[:, :, None], jnp.float32(0.0)), axis=1)
    block_id = jnp.arange(TOKENS, dtype=jnp.int32) // TOK_DEV
    pair_of = jnp.sum(jnp.where(expert_pairs[None, :] == catalog[:, None], catalog[None, :], 0), axis=1).astype(jnp.int32)
    row_total = N_EXPERT * CAP
    padded_tokens = jnp.concatenate([tokens, jnp.zeros((1, D), jnp.bfloat16)], axis=0)
    padded_grad = jnp.concatenate([out_grad.astype(jnp.float32), jnp.zeros((1, D), jnp.float32)], axis=0)
    first_half = (jnp.arange(row_total, dtype=jnp.int32) % CAP) < HALF

    def halves(left, right):
        first_rows = jnp.where(first_half[:, None], left, jnp.zeros_like(left))
        other_rows = jnp.where(first_half[:, None], jnp.zeros_like(left), left)
        first_part = rounded(jnp.dot(first_rows.T, right, preferred_element_type=jnp.float32))
        other_part = rounded(jnp.dot(other_rows.T, right, preferred_element_type=jnp.float32))
        return (first_part + other_part).astype(jnp.bfloat16)

    def per_expert(state_now, expert_id):
        output_acc, grad_acc, inner_dots = state_now
        dest_row = jnp.where(present[:, expert_id] > 0, block_id * CAP + before[:, expert_id], row_total).astype(jnp.int32)
        slot_table = jnp.full((row_total + 1,), TOKENS, jnp.int32).at[dest_row].set(jnp.arange(TOKENS, dtype=jnp.int32))[:row_total]
        rows_in = padded_tokens[slot_table]
        padded_weight = jnp.concatenate([weight_sel[:, expert_id], jnp.zeros((1,), jnp.float32)], axis=0)
        row_weight = padded_weight[slot_table]
        grad_rows = padded_grad[slot_table]
        cot_rows = (row_weight[:, None] * grad_rows).astype(jnp.bfloat16)
        pair_index = pair_of[expert_id]
        w_gate = gate_weight[pair_index]
        w_up = up_weight[pair_index]
        w_down = down_weight[pair_index]
        gate_pre = block_sums(rows_in, w_gate)
        up_pre = block_sums(rows_in, w_up)
        hidden = (jax.nn.silu(gate_pre) * up_pre).astype(jnp.bfloat16)
        expert_out = jnp.dot(hidden, w_down, preferred_element_type=jnp.float32).astype(jnp.bfloat16)
        hidden_grad = back_block_sums(cot_rows, w_down)
        sigmoid_gate = jax.nn.sigmoid(gate_pre)
        up_grad = (hidden_grad * gate_pre * sigmoid_gate).astype(jnp.bfloat16)
        pre_grad = (hidden_grad * up_pre * sigmoid_gate * (1.0 + gate_pre * (1.0 - sigmoid_gate))).astype(jnp.bfloat16)
        row_input_grad = (jnp.dot(pre_grad, w_gate.T, preferred_element_type=jnp.float32) + jnp.dot(up_grad, w_up.T, preferred_element_type=jnp.float32)).astype(jnp.bfloat16)
        grad_gate = halves(rows_in, pre_grad)
        grad_up = halves(rows_in, up_grad)
        grad_down = halves(hidden, cot_rows)
        out_float = expert_out.astype(jnp.float32)
        output_acc = output_acc.at[slot_table].add(row_weight[:, None] * out_float)
        grad_acc = grad_acc.at[slot_table].add(row_input_grad.astype(jnp.float32))
        inner_dots = inner_dots.at[slot_table, expert_id].set(jnp.sum(grad_rows * out_float, axis=1))
        return (output_acc, grad_acc, inner_dots), (grad_gate, grad_up, grad_down)

    start_state = (jnp.zeros((TOKENS + 1, D), jnp.float32), jnp.zeros((TOKENS + 1, D), jnp.float32), jnp.zeros((TOKENS + 1, EXPERTS), jnp.float32))
    final_state, expert_grads = lax.scan(per_expert, start_state, catalog)
    output_acc, grad_acc, inner_dots = final_state
    layer_output = output_acc[:TOKENS].astype(jnp.bfloat16)
    token_grad = grad_acc[:TOKENS].astype(jnp.bfloat16)
    gate_value_grad = jnp.take_along_axis(inner_dots[:TOKENS], route_lists, axis=1)
    slot_experts = expert_pairs[jnp.arange(2 * EXPERTS, dtype=jnp.int32) % EXPERTS]
    gate_weight_grad = expert_grads[0][slot_experts]
    up_weight_grad = expert_grads[1][slot_experts]
    down_weight_grad = expert_grads[2][slot_experts]
    return (layer_output, token_grad, gate_value_grad, gate_weight_grad, up_weight_grad, down_weight_grad)
```

```python
import jax
import jax.numpy as jnp
from jax import lax
from jax.experimental import pallas as pl
from jax.experimental.pallas import tpu as pltpu
from jax.sharding import PartitionSpec as P

F32 = jnp.float32
BF16 = jnp.bfloat16
TOK = 128
WID = 640
FF = 1024
CAP = 72
PAIR = 2 * CAP
GROUPS = 8
ROWS = GROUPS * PAIR
PU = 2 * FF + 128
RW = WID + 128
FAR = 4096.0

UP_SLOT = (2, 4, 6, 1)
DOWN_SLOT = (3, 5, 7, 1)
UP_CHAIN = (1, 7, 5, 3, 0)
DOWN_CHAIN = (1, 6, 4, 2, 0)

S_Z = 0
S_Y = 24
S_CG, S_XG = 32, 36
S_CH, S_XH = 40, 44
S_AX, S_AC = 48, 52
S_BX, S_BC = 56, 60
S_RO, S_RR = 64, 68
S_GD, S_GG = 72, 76
S_ZO = 84
N_SEM = 100


def dot(a, b):
    return jnp.dot(a, b, preferred_element_type=F32)


def dot_nt(a, b):
    return lax.dot_general(a, b, (((1,), (1,)), ((), ())), preferred_element_type=F32)


def dot_tn(a, b):
    return lax.dot_general(a, b, (((0,), (0,)), ((), ())), preferred_element_type=F32)


def layer(
    tok, og, route, gates, pairs, wg_in, wu_in, wd_in,
    out_o, grad_o, sdot_o, gg_o, gu_o, gd_o,
    wgu, wd, tab, tokz, ogz, rows, cot, rows_t, ysend, csend,
    part, crecv, xrecv, hpart, hcrecv, hxrecv, gpre, hid, pu,
    outb, outret, rigb, rigret, gd, gdr, gg, ggr,
    zo_part, zr_part, zo_send, zr_send, zo_recv, zr_recv,
    wsem, ssem, rsem,
):
    dp = lax.axis_index("dp")
    ex = lax.axis_index("expert")
    x, core = dp // 2, dp % 2
    y, z = ex // 8, ex % 8
    own_pair = (y % 2) * 8 + z
    oth_pair = (1 - y % 2) * 8 + z
    shard = dp

    def at(dx=0, dy=0, dz=0, other=False):
        c = 1 - core if other else core
        return (
            ((x + dx) % 4) * 2 + c,
            ((y + dy) % 4) * 8 + (z + dz) % 8,
        )

    def copy(src, dst, sem, device):
        return pltpu.make_async_remote_copy(
            src_ref=src,
            dst_ref=dst,
            send_sem=ssem.at[sem],
            recv_sem=rsem.at[sem],
            device_id=device,
            device_id_type=pl.DeviceIdType.MESH,
        )

    def group(g):
        return pl.ds(pl.multiple_of(g * PAIR, 16), PAIR)

    weights = [
        pltpu.make_async_copy(wg_in, wgu.at[:, 0:FF], wsem.at[0]),
        pltpu.make_async_copy(wu_in, wgu.at[:, FF : 2 * FF], wsem.at[1]),
        pltpu.make_async_copy(wd_in, wd, wsem.at[2]),
    ]
    for w in weights:
        w.start()

    barrier = pltpu.get_barrier_semaphore()
    peers = [at(dz=1), at(dz=-1), at(dy=1), at(dy=-1), at(dy=2)]
    peers += [at(dx=1), at(dx=2), at(dx=3), at(other=True)]
    for peer in peers:
        pl.semaphore_signal(barrier, inc=1, device_id=peer, device_id_type=pl.DeviceIdType.MESH)

    present = jnp.zeros((16, TOK), F32)
    weight = jnp.zeros((16, TOK), F32)
    pair_of = pairs[...]
    for k in range(8):
        named = route[k : k + 1, :] == pair_of
        present = present + jnp.where(named, 1.0, 0.0)
        weight = weight + jnp.where(named, gates[k : k + 1, :], 0.0)
    earlier = lax.broadcasted_iota(jnp.int32, (TOK, TOK), 0) < lax.broadcasted_iota(
        jnp.int32, (TOK, TOK), 1
    )
    before = dot(present.astype(BF16), jnp.where(earlier, 1.0, 0.0).astype(BF16))
    tab[0, 0:16, :] = jnp.where(present > 0.0, before, FAR)
    tab[0, 16:32, :] = weight
    tokz[0:TOK, :] = tok[...]
    ogz[0:TOK, :] = og[...]
    pl.semaphore_wait(barrier, len(peers))

    def block(ref, slot):
        return ref.at[slot] if ref is tab else ref.at[pl.ds(slot * TOK, TOK)]

    arrays = (tab, tokz, ogz)
    lengths = ((4, 3), (4, 3), (3, 4))
    pending = []

    def z_send(a, down, step):
        slots = DOWN_SLOT if down else UP_SLOT
        ref = arrays[a]
        if step == 0:
            src = tok if a == 1 else og if a == 2 else tab.at[0]
        else:
            src = block(ref, slots[step - 1])
        c = copy(
            src, block(ref, slots[step]), S_Z + (a * 2 + down) * 4 + step, at(dz=-1 if down else 1)
        )
        c.start()
        pending.append(c)

    def z_take(a, step):
        for down in (0, 1):
            if step < lengths[a][down]:
                slots = DOWN_SLOT if down else UP_SLOT
                dst = block(arrays[a], slots[step])
                copy(dst, dst, S_Z + (a * 2 + down) * 4 + step, at()).wait_recv()
                if step + 1 < lengths[a][down]:
                    z_send(a, down, step + 1)

    for a in range(3):
        for down in (0, 1):
            z_send(a, down, 0)

    row_no = lax.broadcasted_iota(jnp.int32, (PAIR, 2 * TOK), 0).astype(F32)

    def selection(j, pair):
        place = jnp.concatenate(
            [tab[2 * j, pl.ds(pair, 1), :], tab[2 * j + 1, pl.ds(pair, 1), :] + float(CAP)], axis=1
        )
        return row_no == place

    def weights_of(j, pair):
        return jnp.concatenate(
            [tab[2 * j, pl.ds(pair + 16, 1), :], tab[2 * j + 1, pl.ds(pair + 16, 1), :]], axis=1
        )

    def one_hot(sel):
        return jnp.where(sel, 1.0, 0.0).astype(BF16)

    for step in range(4):
        j = (step + 1) % 4
        dst_group = (4, 6, 5, 7)[step]
        toward = at(dy=-1 if step % 2 else 1)
        z_take(0, step)
        z_take(1, step)
        pick_own = selection(j, own_pair)
        pick_oth = selection(j, oth_pair)
        two = tokz[2 * TOK * j : 2 * TOK * (j + 1), :]
        ysend[j] = dot(one_hot(pick_oth), two).astype(BF16)
        c = copy(ysend.at[j], rows.at[group(dst_group)], S_Y + step, toward)
        c.start()
        pending.append(c)
        rows[j * PAIR : (j + 1) * PAIR, :] = dot(one_hot(pick_own), two).astype(BF16)
        z_take(2, step)
        two = ogz[2 * TOK * j : 2 * TOK * (j + 1), :]
        scale = jnp.sum(jnp.where(pick_oth, weights_of(j, oth_pair), 0.0), axis=1, keepdims=True)
        csend[j] = (dot(one_hot(pick_oth), two) * scale).astype(BF16)
        c = copy(csend.at[j], cot.at[group(dst_group)], S_Y + 4 + step, toward)
        c.start()
        pending.append(c)
        scale = jnp.sum(jnp.where(pick_own, weights_of(j, own_pair), 0.0), axis=1, keepdims=True)
        cot[j * PAIR : (j + 1) * PAIR, :] = (dot(one_hot(pick_own), two) * scale).astype(BF16)

    def reduce_terms(tiles, term, mine, from_core, from_x, s_core, s_x):
        def step(i, _):
            @pl.when(i < 4)
            def _():
                chip = (x + 1 + i) % 4
                span = pl.ds(pl.multiple_of(chip * 2 * PAIR, 16), 2 * PAIR)

                def tile(n, _):
                    cols = pl.ds(pl.multiple_of(n * 512, 512), 512)
                    mine[span, cols] = term(span, cols).astype(BF16)
                    return 0

                lax.fori_loop(0, tiles, tile, 0)
                copy(
                    mine.at[group(chip * 2 + 1 - core)],
                    from_core.at[chip],
                    s_core + i,
                    at(other=True),
                ).start()

            @pl.when(i >= 1)
            def _():
                chip = (x + i) % 4
                copy(from_core.at[chip], from_core.at[chip], s_core + i - 1, at()).wait_recv()
                g = group(chip * 2 + core)
                mine[g, :] = (mine[g, :].astype(F32) + from_core[chip].astype(F32)).astype(BF16)

                @pl.when(i < 4)
                def _():
                    copy(
                        mine.at[g], from_x.at[i - 1], s_x + i - 1, (chip * 2 + core, ex)
                    ).start()

            return 0

        lax.fori_loop(0, 5, step, 0)

    for step in range(4):
        dst = rows.at[group((4, 6, 5, 7)[step])]
        copy(dst, dst, S_Y + step, at()).wait_recv()
    weights[0].wait()
    weights[1].wait()
    reduce_terms(
        4, lambda span, cols: dot(rows[span, :], wgu[:, cols]), part, crecv, xrecv, S_CG, S_XG
    )
    for step in range(4):
        dst = cot.at[group((4, 6, 5, 7)[step])]
        copy(dst, dst, S_Y + 4 + step, at()).wait_recv()
    weights[2].wait()
    reduce_terms(
        2, lambda span, cols: dot_nt(cot[span, :], wd[cols, :]), hpart, hcrecv, hxrecv, S_CH, S_XH
    )

    mine = group(shard)
    for i in range(3):
        copy(xrecv.at[i], xrecv.at[i], S_XG + i, at()).wait_recv()

    def total(src, recv, cols):
        v = src[mine, cols].astype(F32)
        for i in range(3):
            v = v + recv[i, :, cols].astype(F32)
        return v

    def forward(n, _):
        cols = pl.ds(pl.multiple_of(n * 256, 256), 256)
        more = pl.ds(pl.multiple_of(FF + n * 256, 256), 256)
        gate_pre = total(part, xrecv, cols)
        up_pre = total(part, xrecv, more)
        gpre[:, cols] = gate_pre
        gpre[:, more] = up_pre
        hid[mine, cols] = (gate_pre * jax.nn.sigmoid(gate_pre) * up_pre).astype(BF16)
        return 0

    lax.fori_loop(0, 4, forward, 0)

    def spread(ref, s_x, s_core):
        for i in range(3):
            copy(ref.at[mine], ref.at[mine], s_x + i, at(dx=1 + i)).start()
        copy(ref.at[mine], ref.at[mine], s_core + 3, at(other=True)).start()

    def relay(ref, s_x, s_core):
        for i in range(3):
            g = ref.at[group(((x - 1 - i) % 4) * 2 + core)]
            copy(g, g, s_x + i, at()).wait_recv()
            copy(g, g, s_core + i, at(other=True)).start()
        for i in range(4):
            g = ref.at[group(((x - 1 - i) % 4) * 2 + 1 - core)]
            copy(g, g, s_core + i, at()).wait_recv()

    def spread_done(ref, s_x, s_core):
        g = ref.at[mine]
        for i in range(3):
            copy(g, g, s_x + i, at()).wait_send()
        for i in range(4):
            copy(g, g, s_core + i, at()).wait_send()

    spread(hid, S_AX, S_AC)
    for i in range(3):
        copy(hxrecv.at[i], hxrecv.at[i], S_XH + i, at()).wait_recv()

    def backward(n, acc):
        cols = pl.ds(pl.multiple_of(n * 256, 256), 256)
        more = pl.ds(pl.multiple_of(FF + n * 256, 256), 256)
        gate_pre = gpre[:, cols]
        up_pre = gpre[:, more]
        back = total(hpart, hxrecv, cols)
        s = jax.nn.sigmoid(gate_pre)
        act = gate_pre * s
        pu[mine, more] = (back * act).astype(BF16)
        pu[mine, cols] = (back * up_pre * s * (1.0 + gate_pre * (1.0 - s))).astype(BF16)
        return acc + jnp.sum(back * act * up_pre, axis=1, keepdims=True)

    sdot = lax.fori_loop(0, 4, backward, jnp.zeros((PAIR, 1), F32))
    sdot_hi = sdot.astype(BF16).astype(F32)
    lane = lax.broadcasted_iota(jnp.int32, (PAIR, 128), 1)
    slab = jnp.where(lane == own_pair, sdot_hi, 0.0) + jnp.where(
        lane == own_pair + 16, sdot - sdot_hi, 0.0
    )
    pu[mine, 2 * FF : PU] = slab.astype(BF16)
    spread(pu, S_BX, S_BC)
    rows_t[...] = rows[...].T

    relay(hid, S_AX, S_AC)
    back_to = ((4, 1, -1), (5, 3, -1), (6, 2, 1), (7, 0, 1))

    def expert_out(m, _):
        span = pl.ds(pl.multiple_of(((m + 2) % 4) * 2 * PAIR, 16), 2 * PAIR)
        outb[span, :] = dot(hid[span, :], wd[...]).astype(BF16)
        return 0

    lax.fori_loop(0, 4, expert_out, 0)
    for n, (g, j, dy) in enumerate(back_to):
        c = copy(outb.at[group(g)], outret.at[j], S_RO + n, at(dy=dy))
        c.start()
        pending.append(c)

    def down_grad(n, _):
        cols = pl.ds(pl.multiple_of(n * 256, 256), 256)
        gd[n] = dot_tn(hid[:, cols], cot[...]).astype(BF16)
        copy(gd.at[n], gdr.at[n], S_GD + n, at(dy=2)).start()
        return 0

    lax.fori_loop(0, 4, down_grad, 0)

    relay(pu, S_BX, S_BC)

    def input_grad(m, _):
        span = pl.ds(pl.multiple_of(((m + 2) % 4) * 2 * PAIR, 16), 2 * PAIR)
        rigb[span, 0:WID] = dot_nt(pu[span, 0 : 2 * FF], wgu[...]).astype(BF16)
        rigb[span, WID:RW] = pu[span, 2 * FF : PU]
        return 0

    lax.fori_loop(0, 4, input_grad, 0)
    for n, (g, j, dy) in enumerate(back_to):
        c = copy(rigb.at[group(g)], rigret.at[j], S_RR + n, at(dy=dy))
        c.start()
        pending.append(c)

    def in_grad(n, _):
        cols = pl.ds(pl.multiple_of(n * 256, 256), 256)
        gg[n] = dot(rows_t[...], pu[:, cols]).astype(BF16)
        copy(gg.at[n], ggr.at[n], S_GG + n, at(dy=2)).start()
        return 0

    lax.fori_loop(0, 8, in_grad, 0)

    for n, (g, j, dy) in enumerate(back_to):
        copy(outret.at[j], outret.at[j], S_RO + n, at()).wait_recv()
        copy(rigret.at[j], rigret.at[j], S_RR + n, at()).wait_recv()
    for j in range(4):
        outs = jnp.zeros((2 * TOK, WID), F32)
        grads = jnp.zeros((2 * TOK, RW), F32)
        for pair, o, r in (
            (own_pair, outb[j * PAIR : (j + 1) * PAIR, :], rigb[j * PAIR : (j + 1) * PAIR, :]),
            (oth_pair, outret[j], rigret[j]),
        ):
            sel = selection(j, pair)
            w = jnp.where(sel, weights_of(j, pair), 0.0)
            hi = w.astype(BF16)
            lo = (w - hi.astype(F32)).astype(BF16)
            outs = outs + dot_tn(hi, o) + dot_tn(lo, o)
            grads = grads + dot_tn(one_hot(sel), r)
        zo_part[2 * j] = outs[0:TOK]
        zo_part[2 * j + 1] = outs[TOK:]
        zr_part[2 * j] = grads[0:TOK]
        zr_part[2 * j + 1] = grads[TOK:]

    chains = []
    for a, (own, send, recv) in enumerate(
        ((zo_part, zo_send, zo_recv), (zr_part, zr_send, zr_recv))
    ):
        for down in (0, 1):
            slots = DOWN_CHAIN if down else UP_CHAIN
            if down != a:
                slots = slots[1:]
            chains.append((own, send, recv, down, slots, S_ZO + (a * 2 + down) * 4))
    for step in range(5):
        for own, send, recv, down, slots, sem in chains:
            if step >= len(slots) - 1:
                continue
            v = own[slots[step]]
            if step:
                prev = recv.at[down * 4 + step - 1]
                copy(prev, prev, sem + step - 1, at()).wait_recv()
                v = v + prev[...].astype(F32)
            send[down * 4 + step] = v.astype(BF16)
            c = copy(
                send.at[down * 4 + step],
                recv.at[down * 4 + step],
                sem + step,
                at(dz=-1 if down else 1),
            )
            c.start()
            pending.append(c)
    finals = []
    for a in (0, 1):
        own = chains[2 * a][0]
        v = own[0]
        for own, send, recv, down, slots, sem in chains[2 * a : 2 * a + 2]:
            prev = recv.at[down * 4 + len(slots) - 2]
            copy(prev, prev, sem + len(slots) - 2, at()).wait_recv()
            v = v + prev[...].astype(F32)
        finals.append(v)
    out_o[...] = finals[0].astype(BF16)
    grad_o[...] = finals[1][:, 0:WID].astype(BF16)
    sdot_o[...] = finals[1][:, WID:RW]

    def add_down(n, _):
        copy(gdr.at[n], gdr.at[n], S_GD + n, at()).wait_recv()
        gd_o[pl.ds(pl.multiple_of(n * 256, 256), 256), :] = (
            gd[n].astype(F32) + gdr[n].astype(F32)
        ).astype(BF16)
        return 0

    lax.fori_loop(0, 4, add_down, 0)

    def add_in(out, base):
        def body(n, _):
            m = base + n
            copy(ggr.at[m], ggr.at[m], S_GG + m, at()).wait_recv()
            out[:, pl.ds(pl.multiple_of(n * 256, 256), 256)] = (
                gg[m].astype(F32) + ggr[m].astype(F32)
            ).astype(BF16)
            return 0

        lax.fori_loop(0, 4, body, 0)

    add_in(gg_o, 0)
    add_in(gu_o, 4)

    for c in pending:
        c.wait_send()
    for i in range(4):
        copy(crecv.at[i], crecv.at[i], S_CG + i, at()).wait_send()
        copy(hcrecv.at[i], hcrecv.at[i], S_CH + i, at()).wait_send()
        copy(gd.at[i], gd.at[i], S_GD + i, at()).wait_send()
    for i in range(3):
        copy(xrecv.at[i], xrecv.at[i], S_XG + i, at()).wait_send()
        copy(hxrecv.at[i], hxrecv.at[i], S_XH + i, at()).wait_send()
    for i in range(8):
        copy(gg.at[i], gg.at[i], S_GG + i, at()).wait_send()
    spread_done(hid, S_AX, S_AC)
    spread_done(pu, S_BX, S_BC)


def shards(tokens, out_grad, gate_values, route_lists, expert_pairs, gate_weight, up_weight, down_weight):
    vmem = pl.BlockSpec(memory_space=pltpu.VMEM)
    hbm = pl.BlockSpec(memory_space=pl.ANY)
    sds = jax.ShapeDtypeStruct
    out, grad, sdot, gg, gu, gd = pl.pallas_call(
        layer,
        name="routed_layer",
        out_shape=(
            sds((TOK, WID), BF16),
            sds((TOK, WID), BF16),
            sds((TOK, 128), F32),
            sds((WID, FF), BF16),
            sds((WID, FF), BF16),
            sds((FF, WID), BF16),
        ),
        in_specs=[vmem] * 5 + [hbm] * 3,
        out_specs=(vmem,) * 6,
        scratch_shapes=[
            pltpu.VMEM((WID, 2 * FF), BF16),
            pltpu.VMEM((FF, WID), BF16),
            pltpu.VMEM((8, 32, TOK), F32),
            pltpu.VMEM((8 * TOK, WID), BF16),
            pltpu.VMEM((8 * TOK, WID), BF16),
            pltpu.VMEM((ROWS, WID), BF16),
            pltpu.VMEM((ROWS, WID), BF16),
            pltpu.VMEM((WID, ROWS), BF16),
            pltpu.VMEM((4, PAIR, WID), BF16),
            pltpu.VMEM((4, PAIR, WID), BF16),
            pltpu.VMEM((ROWS, 2 * FF), BF16),
            pltpu.VMEM((4, PAIR, 2 * FF), BF16),
            pltpu.VMEM((3, PAIR, 2 * FF), BF16),
            pltpu.VMEM((ROWS, FF), BF16),
            pltpu.VMEM((4, PAIR, FF), BF16),
            pltpu.VMEM((3, PAIR, FF), BF16),
            pltpu.VMEM((PAIR, 2 * FF), F32),
            pltpu.VMEM((ROWS, FF), BF16),
            pltpu.VMEM((ROWS, PU), BF16),
            pltpu.VMEM((ROWS, WID), BF16),
            pltpu.VMEM((4, PAIR, WID), BF16),
            pltpu.VMEM((ROWS, RW), BF16),
            pltpu.VMEM((4, PAIR, RW), BF16),
            pltpu.VMEM((4, 256, WID), BF16),
            pltpu.VMEM((4, 256, WID), BF16),
            pltpu.VMEM((8, WID, 256), BF16),
            pltpu.VMEM((8, WID, 256), BF16),
            pltpu.VMEM((8, TOK, WID), F32),
            pltpu.VMEM((8, TOK, RW), F32),
            pltpu.VMEM((8, TOK, WID), BF16),
            pltpu.VMEM((8, TOK, RW), BF16),
            pltpu.VMEM((8, TOK, WID), BF16),
            pltpu.VMEM((8, TOK, RW), BF16),
            pltpu.SemaphoreType.DMA((3,)),
            pltpu.SemaphoreType.DMA((N_SEM,)),
            pltpu.SemaphoreType.DMA((N_SEM,)),
        ],
        compiler_params=pltpu.CompilerParams(
            collective_id=0, has_side_effects=True, vmem_limit_bytes=67043328
        ),
    )(
        tokens,
        out_grad,
        route_lists.T,
        gate_values.T,
        expert_pairs.reshape(16, 1),
        gate_weight[0],
        up_weight[0],
        down_weight[0],
    )
    dots = sdot[:, 0:16] + sdot[:, 16:32]
    named = route_lists[:, :, None] == expert_pairs[None, None, :]
    gate_value_grad = jnp.sum(jnp.where(named, dots[:, None, :], 0.0), axis=2) / gate_values
    return out, grad, gate_value_grad, gg[None], gu[None], gd[None]


def solution(mesh):
    placed = (
        P("expert", "dp"),
        P("expert", "dp"),
        P("expert", None),
        P("expert", None),
        P(),
        P("expert", "dp", None),
        P("expert", "dp", None),
        P("expert", None, "dp"),
    )
    return jax.shard_map(
        shards,
        mesh=mesh,
        in_specs=placed,
        out_specs=(
            P("expert", "dp"),
            P("expert", "dp"),
            P("expert", None),
            P("expert", "dp", None),
            P("expert", "dp", None),
            P("expert", None, "dp"),
        ),
        check_vma=False,
    )
```

```python
import jax
import jax.numpy as jnp
from jax import lax
from jax.experimental import pallas as pl
from jax.experimental.pallas import tpu as pltpu
from jax.sharding import PartitionSpec as P

F32 = jnp.float32
BF16 = jnp.bfloat16
TOK = 128
WID = 640
FF = 1024
CAP = 72
PAIR = 2 * CAP
GROUPS = 8
ROWS = GROUPS * PAIR
PU = 2 * FF + 128
RW = WID + 128
FAR = 4096.0

UP_SLOT = (2, 4, 6, 1)
DOWN_SLOT = (3, 5, 7, 1)
UP_CHAIN = (1, 7, 5, 3, 0)
DOWN_CHAIN = (1, 6, 4, 2, 0)

S_Z = 0
S_Y = 24
S_CG, S_XG = 32, 36
S_CH, S_XH = 40, 44
S_AX, S_AC = 48, 52
S_BX, S_BC = 56, 60
S_RO, S_RR = 64, 68
S_GD, S_GG = 72, 76
S_ZO = 84
S_RD, S_RG = 100, 104
N_SEM = 112


def dot(a, b):
    return jnp.dot(a, b, preferred_element_type=F32)


def dot_nt(a, b):
    return lax.dot_general(a, b, (((1,), (1,)), ((), ())), preferred_element_type=F32)


def dot_tn(a, b):
    return lax.dot_general(a, b, (((0,), (0,)), ((), ())), preferred_element_type=F32)


def layer(
    tok, og, route, gates, pairs, wg_in, wu_in, wd_in,
    out_o, grad_o, sdot_o, gg_o, gu_o, gd_o,
    wgu, wd, tab, tokz, ogz, rows, cot, rows_t, ysend, csend,
    part, crecv, xrecv, hpart, hcrecv, hxrecv, gpre, hid, pu,
    outb, outret, rigb, rigret, gd, gdr, gg, ggr, gd_via, gg_via,
    zo_part, zr_part, zo_send, zr_send, zo_recv, zr_recv,
    wsem, ssem, rsem,
):
    dp = lax.axis_index("dp")
    ex = lax.axis_index("expert")
    x, core = dp // 2, dp % 2
    y, z = ex // 8, ex % 8
    own_pair = (y % 2) * 8 + z
    oth_pair = (1 - y % 2) * 8 + z
    shard = dp

    def at(dx=0, dy=0, dz=0, other=False):
        c = 1 - core if other else core
        return (
            ((x + dx) % 4) * 2 + c,
            ((y + dy) % 4) * 8 + (z + dz) % 8,
        )

    def copy(src, dst, sem, device):
        return pltpu.make_async_remote_copy(
            src_ref=src,
            dst_ref=dst,
            send_sem=ssem.at[sem],
            recv_sem=rsem.at[sem],
            device_id=device,
            device_id_type=pl.DeviceIdType.MESH,
        )

    def group(g):
        return pl.ds(pl.multiple_of(g * PAIR, 16), PAIR)

    weights = [
        pltpu.make_async_copy(wg_in, wgu.at[:, 0:FF], wsem.at[0]),
        pltpu.make_async_copy(wu_in, wgu.at[:, FF : 2 * FF], wsem.at[1]),
        pltpu.make_async_copy(wd_in, wd, wsem.at[2]),
    ]
    for w in weights:
        w.start()

    barrier = pltpu.get_barrier_semaphore()
    peers = [at(dz=1), at(dz=-1), at(dy=1), at(dy=-1)]
    peers += [at(dx=1), at(dx=2), at(dx=3), at(other=True)]
    for peer in peers:
        pl.semaphore_signal(barrier, inc=1, device_id=peer, device_id_type=pl.DeviceIdType.MESH)

    present = jnp.zeros((16, TOK), F32)
    weight = jnp.zeros((16, TOK), F32)
    pair_of = pairs[...]
    for k in range(8):
        named = route[k : k + 1, :] == pair_of
        present = present + jnp.where(named, 1.0, 0.0)
        weight = weight + jnp.where(named, gates[k : k + 1, :], 0.0)
    earlier = lax.broadcasted_iota(jnp.int32, (TOK, TOK), 0) < lax.broadcasted_iota(
        jnp.int32, (TOK, TOK), 1
    )
    before = dot(present.astype(BF16), jnp.where(earlier, 1.0, 0.0).astype(BF16))
    tab[0, 0:16, :] = jnp.where(present > 0.0, before, FAR)
    tab[0, 16:32, :] = weight
    tokz[0:TOK, :] = tok[...]
    ogz[0:TOK, :] = og[...]
    pl.semaphore_wait(barrier, len(peers))

    def block(ref, slot):
        return ref.at[slot] if ref is tab else ref.at[pl.ds(slot * TOK, TOK)]

    arrays = (tab, tokz, ogz)
    lengths = ((4, 3), (4, 3), (3, 4))
    pending = []

    def z_send(a, down, step):
        slots = DOWN_SLOT if down else UP_SLOT
        ref = arrays[a]
        if step == 0:
            src = tok if a == 1 else og if a == 2 else tab.at[0]
        else:
            src = block(ref, slots[step - 1])
        c = copy(
            src, block(ref, slots[step]), S_Z + (a * 2 + down) * 4 + step, at(dz=-1 if down else 1)
        )
        c.start()
        pending.append(c)

    def z_take(a, step):
        for down in (0, 1):
            if step < lengths[a][down]:
                slots = DOWN_SLOT if down else UP_SLOT
                dst = block(arrays[a], slots[step])
                copy(dst, dst, S_Z + (a * 2 + down) * 4 + step, at()).wait_recv()
                if step + 1 < lengths[a][down]:
                    z_send(a, down, step + 1)

    for a in range(3):
        for down in (0, 1):
            z_send(a, down, 0)

    row_no = lax.broadcasted_iota(jnp.int32, (PAIR, 2 * TOK), 0).astype(F32)

    def selection(j, pair):
        place = jnp.concatenate(
            [tab[2 * j, pl.ds(pair, 1), :], tab[2 * j + 1, pl.ds(pair, 1), :] + float(CAP)], axis=1
        )
        return row_no == place

    def weights_of(j, pair):
        return jnp.concatenate(
            [tab[2 * j, pl.ds(pair + 16, 1), :], tab[2 * j + 1, pl.ds(pair + 16, 1), :]], axis=1
        )

    def one_hot(sel):
        return jnp.where(sel, 1.0, 0.0).astype(BF16)

    for step in range(4):
        j = (step + 1) % 4
        dst_group = (4, 6, 5, 7)[step]
        toward = at(dy=-1 if step % 2 else 1)
        z_take(0, step)
        z_take(1, step)
        pick_own = selection(j, own_pair)
        pick_oth = selection(j, oth_pair)
        two = tokz[2 * TOK * j : 2 * TOK * (j + 1), :]
        ysend[j] = dot(one_hot(pick_oth), two).astype(BF16)
        c = copy(ysend.at[j], rows.at[group(dst_group)], S_Y + step, toward)
        c.start()
        pending.append(c)
        rows[j * PAIR : (j + 1) * PAIR, :] = dot(one_hot(pick_own), two).astype(BF16)
        z_take(2, step)
        two = ogz[2 * TOK * j : 2 * TOK * (j + 1), :]
        scale = jnp.sum(jnp.where(pick_oth, weights_of(j, oth_pair), 0.0), axis=1, keepdims=True)
        csend[j] = (dot(one_hot(pick_oth), two) * scale).astype(BF16)
        c = copy(csend.at[j], cot.at[group(dst_group)], S_Y + 4 + step, toward)
        c.start()
        pending.append(c)
        scale = jnp.sum(jnp.where(pick_own, weights_of(j, own_pair), 0.0), axis=1, keepdims=True)
        cot[j * PAIR : (j + 1) * PAIR, :] = (dot(one_hot(pick_own), two) * scale).astype(BF16)

    def reduce_terms(tiles, term, mine, from_core, from_x, s_core, s_x):
        def step(i, _):
            @pl.when(i < 4)
            def _():
                chip = (x + 1 + i) % 4
                span = pl.ds(pl.multiple_of(chip * 2 * PAIR, 16), 2 * PAIR)

                def tile(n, _):
                    cols = pl.ds(pl.multiple_of(n * 512, 512), 512)
                    mine[span, cols] = term(span, cols).astype(BF16)
                    return 0

                lax.fori_loop(0, tiles, tile, 0)
                copy(
                    mine.at[group(chip * 2 + 1 - core)],
                    from_core.at[chip],
                    s_core + i,
                    at(other=True),
                ).start()

            @pl.when(i >= 1)
            def _():
                chip = (x + i) % 4
                copy(from_core.at[chip], from_core.at[chip], s_core + i - 1, at()).wait_recv()
                g = group(chip * 2 + core)
                mine[g, :] = (mine[g, :].astype(F32) + from_core[chip].astype(F32)).astype(BF16)

                @pl.when(i < 4)
                def _():
                    copy(
                        mine.at[g], from_x.at[i - 1], s_x + i - 1, (chip * 2 + core, ex)
                    ).start()

            return 0

        lax.fori_loop(0, 5, step, 0)

    for step in range(4):
        dst = rows.at[group((4, 6, 5, 7)[step])]
        copy(dst, dst, S_Y + step, at()).wait_recv()
    weights[0].wait()
    weights[1].wait()
    reduce_terms(
        4, lambda span, cols: dot(rows[span, :], wgu[:, cols]), part, crecv, xrecv, S_CG, S_XG
    )
    for step in range(4):
        dst = cot.at[group((4, 6, 5, 7)[step])]
        copy(dst, dst, S_Y + 4 + step, at()).wait_recv()
    weights[2].wait()
    reduce_terms(
        2, lambda span, cols: dot_nt(cot[span, :], wd[cols, :]), hpart, hcrecv, hxrecv, S_CH, S_XH
    )

    mine = group(shard)
    for i in range(3):
        copy(xrecv.at[i], xrecv.at[i], S_XG + i, at()).wait_recv()

    def total(src, recv, cols):
        v = src[mine, cols].astype(F32)
        for i in range(3):
            v = v + recv[i, :, cols].astype(F32)
        return v

    def forward(n, _):
        cols = pl.ds(pl.multiple_of(n * 256, 256), 256)
        more = pl.ds(pl.multiple_of(FF + n * 256, 256), 256)
        gate_pre = total(part, xrecv, cols)
        up_pre = total(part, xrecv, more)
        gpre[:, cols] = gate_pre
        gpre[:, more] = up_pre
        hid[mine, cols] = (gate_pre * jax.nn.sigmoid(gate_pre) * up_pre).astype(BF16)
        return 0

    lax.fori_loop(0, 4, forward, 0)

    def spread(ref, s_x, s_core):
        for i in range(3):
            copy(ref.at[mine], ref.at[mine], s_x + i, at(dx=1 + i)).start()
        copy(ref.at[mine], ref.at[mine], s_core + 3, at(other=True)).start()

    def relay(ref, s_x, s_core):
        for i in range(3):
            g = ref.at[group(((x - 1 - i) % 4) * 2 + core)]
            copy(g, g, s_x + i, at()).wait_recv()
            copy(g, g, s_core + i, at(other=True)).start()
        for i in range(4):
            g = ref.at[group(((x - 1 - i) % 4) * 2 + 1 - core)]
            copy(g, g, s_core + i, at()).wait_recv()

    def spread_done(ref, s_x, s_core):
        g = ref.at[mine]
        for i in range(3):
            copy(g, g, s_x + i, at()).wait_send()
        for i in range(4):
            copy(g, g, s_core + i, at()).wait_send()

    spread(hid, S_AX, S_AC)
    for i in range(3):
        copy(hxrecv.at[i], hxrecv.at[i], S_XH + i, at()).wait_recv()

    def backward(n, acc):
        cols = pl.ds(pl.multiple_of(n * 256, 256), 256)
        more = pl.ds(pl.multiple_of(FF + n * 256, 256), 256)
        gate_pre = gpre[:, cols]
        up_pre = gpre[:, more]
        back = total(hpart, hxrecv, cols)
        s = jax.nn.sigmoid(gate_pre)
        act = gate_pre * s
        pu[mine, more] = (back * act).astype(BF16)
        pu[mine, cols] = (back * up_pre * s * (1.0 + gate_pre * (1.0 - s))).astype(BF16)
        return acc + jnp.sum(back * act * up_pre, axis=1, keepdims=True)

    sdot = lax.fori_loop(0, 4, backward, jnp.zeros((PAIR, 1), F32))
    sdot_hi = sdot.astype(BF16).astype(F32)
    lane = lax.broadcasted_iota(jnp.int32, (PAIR, 128), 1)
    slab = jnp.where(lane == own_pair, sdot_hi, 0.0) + jnp.where(
        lane == own_pair + 16, sdot - sdot_hi, 0.0
    )
    pu[mine, 2 * FF : PU] = slab.astype(BF16)
    spread(pu, S_BX, S_BC)
    rows_t[...] = rows[...].T

    def pass_on(via, end, s_via, s_end, tiles):
        for n in tiles:
            copy(via.at[n], via.at[n], s_via + n, at()).wait_recv()
            copy(via.at[n], end.at[n], s_end + n, at(dy=1 - 2 * (n % 2))).start()

    relay(hid, S_AX, S_AC)
    back_to = ((4, 1, -1), (5, 3, -1), (6, 2, 1), (7, 0, 1))

    def expert_out(m, _):
        span = pl.ds(pl.multiple_of(((m + 2) % 4) * 2 * PAIR, 16), 2 * PAIR)
        outb[span, :] = dot(hid[span, :], wd[...]).astype(BF16)
        return 0

    lax.fori_loop(0, 4, expert_out, 0)
    for n, (g, j, dy) in enumerate(back_to):
        c = copy(outb.at[group(g)], outret.at[j], S_RO + n, at(dy=dy))
        c.start()
        pending.append(c)

    def down_grad(n, _):
        cols = pl.ds(pl.multiple_of(n * 256, 256), 256)
        gd[n] = dot_tn(hid[:, cols], cot[...]).astype(BF16)
        copy(gd.at[n], gd_via.at[n], S_RD + n, at(dy=1 - 2 * (n % 2))).start()
        return 0

    lax.fori_loop(0, 4, down_grad, 0)

    relay(pu, S_BX, S_BC)
    pass_on(gd_via, gdr, S_RD, S_GD, (0, 1))

    def input_grad(m, _):
        span = pl.ds(pl.multiple_of(((m + 2) % 4) * 2 * PAIR, 16), 2 * PAIR)
        rigb[span, 0:WID] = dot_nt(pu[span, 0 : 2 * FF], wgu[...]).astype(BF16)
        rigb[span, WID:RW] = pu[span, 2 * FF : PU]
        return 0

    lax.fori_loop(0, 4, input_grad, 0)
    for n, (g, j, dy) in enumerate(back_to):
        c = copy(rigb.at[group(g)], rigret.at[j], S_RR + n, at(dy=dy))
        c.start()
        pending.append(c)

    def in_grad(n, _):
        cols = pl.ds(pl.multiple_of(n * 256, 256), 256)
        gg[n] = dot(rows_t[...], pu[:, cols]).astype(BF16)
        copy(gg.at[n], gg_via.at[n], S_RG + n, at(dy=1 - 2 * (n % 2))).start()
        return 0

    lax.fori_loop(0, 8, in_grad, 0)
    pass_on(gd_via, gdr, S_RD, S_GD, (2, 3))

    for n, (g, j, dy) in enumerate(back_to):
        copy(outret.at[j], outret.at[j], S_RO + n, at()).wait_recv()
        copy(rigret.at[j], rigret.at[j], S_RR + n, at()).wait_recv()
    for j in range(4):
        outs = jnp.zeros((2 * TOK, WID), F32)
        grads = jnp.zeros((2 * TOK, RW), F32)
        for pair, o, r in (
            (own_pair, outb[j * PAIR : (j + 1) * PAIR, :], rigb[j * PAIR : (j + 1) * PAIR, :]),
            (oth_pair, outret[j], rigret[j]),
        ):
            sel = selection(j, pair)
            w = jnp.where(sel, weights_of(j, pair), 0.0)
            hi = w.astype(BF16)
            lo = (w - hi.astype(F32)).astype(BF16)
            outs = outs + dot_tn(hi, o) + dot_tn(lo, o)
            grads = grads + dot_tn(one_hot(sel), r)
        zo_part[2 * j] = outs[0:TOK]
        zo_part[2 * j + 1] = outs[TOK:]
        zr_part[2 * j] = grads[0:TOK]
        zr_part[2 * j + 1] = grads[TOK:]

    chains = []
    for a, (own, send, recv) in enumerate(
        ((zo_part, zo_send, zo_recv), (zr_part, zr_send, zr_recv))
    ):
        for down in (0, 1):
            slots = DOWN_CHAIN if down else UP_CHAIN
            if down != a:
                slots = slots[1:]
            chains.append((own, send, recv, down, slots, S_ZO + (a * 2 + down) * 4))
    for step in range(5):
        for own, send, recv, down, slots, sem in chains:
            if step >= len(slots) - 1:
                continue
            v = own[slots[step]]
            if step:
                prev = recv.at[down * 4 + step - 1]
                copy(prev, prev, sem + step - 1, at()).wait_recv()
                v = v + prev[...].astype(F32)
            send[down * 4 + step] = v.astype(BF16)
            c = copy(
                send.at[down * 4 + step],
                recv.at[down * 4 + step],
                sem + step,
                at(dz=-1 if down else 1),
            )
            c.start()
            pending.append(c)
        if step < 4:
            pass_on(gg_via, ggr, S_RG, S_GG, (2 * step, 2 * step + 1))
    finals = []
    for a in (0, 1):
        own = chains[2 * a][0]
        v = own[0]
        for own, send, recv, down, slots, sem in chains[2 * a : 2 * a + 2]:
            prev = recv.at[down * 4 + len(slots) - 2]
            copy(prev, prev, sem + len(slots) - 2, at()).wait_recv()
            v = v + prev[...].astype(F32)
        finals.append(v)
    out_o[...] = finals[0].astype(BF16)
    grad_o[...] = finals[1][:, 0:WID].astype(BF16)
    sdot_o[...] = finals[1][:, WID:RW]

    def store_down(n):
        span = pl.ds(pl.multiple_of(n * 256, 256), 256)
        return pltpu.make_async_copy(gdr.at[n], gd_o.at[span, :], wsem.at[3 + n])

    def store_in(out, m, n):
        cols = pl.ds(pl.multiple_of(n * 256, 256), 256)
        return pltpu.make_async_copy(ggr.at[m], out.at[:, cols], wsem.at[7 + m])

    def add_down(n, _):
        copy(gdr.at[n], gdr.at[n], S_GD + n, at()).wait_recv()
        gdr[n] = (gd[n].astype(F32) + gdr[n].astype(F32)).astype(BF16)
        store_down(n).start()
        return 0

    lax.fori_loop(0, 4, add_down, 0)

    def add_in(out, base):
        def body(n, _):
            m = base + n
            copy(ggr.at[m], ggr.at[m], S_GG + m, at()).wait_recv()
            ggr[m] = (gg[m].astype(F32) + ggr[m].astype(F32)).astype(BF16)
            store_in(out, m, n).start()
            return 0

        lax.fori_loop(0, 4, body, 0)

    add_in(gg_o, 0)
    add_in(gu_o, 4)

    for n in range(4):
        store_down(n).wait()
        store_in(gg_o, n, n).wait()
        store_in(gu_o, 4 + n, n).wait()

    for c in pending:
        c.wait_send()
    for i in range(4):
        copy(crecv.at[i], crecv.at[i], S_CG + i, at()).wait_send()
        copy(hcrecv.at[i], hcrecv.at[i], S_CH + i, at()).wait_send()
        copy(gd.at[i], gd.at[i], S_RD + i, at()).wait_send()
        copy(gd_via.at[i], gd_via.at[i], S_GD + i, at()).wait_send()
    for i in range(3):
        copy(xrecv.at[i], xrecv.at[i], S_XG + i, at()).wait_send()
        copy(hxrecv.at[i], hxrecv.at[i], S_XH + i, at()).wait_send()
    for i in range(8):
        copy(gg.at[i], gg.at[i], S_RG + i, at()).wait_send()
        copy(gg_via.at[i], gg_via.at[i], S_GG + i, at()).wait_send()
    spread_done(hid, S_AX, S_AC)
    spread_done(pu, S_BX, S_BC)


def shards(tokens, out_grad, gate_values, route_lists, expert_pairs, gate_weight, up_weight, down_weight):
    vmem = pl.BlockSpec(memory_space=pltpu.VMEM)
    hbm = pl.BlockSpec(memory_space=pl.ANY)
    sds = jax.ShapeDtypeStruct
    out, grad, sdot, gg, gu, gd = pl.pallas_call(
        layer,
        name="routed_layer",
        out_shape=(
            sds((TOK, WID), BF16),
            sds((TOK, WID), BF16),
            sds((TOK, 128), F32),
            sds((WID, FF), BF16),
            sds((WID, FF), BF16),
            sds((FF, WID), BF16),
        ),
        in_specs=[vmem] * 5 + [hbm] * 3,
        out_specs=(vmem,) * 3 + (hbm,) * 3,
        scratch_shapes=[
            pltpu.VMEM((WID, 2 * FF), BF16),
            pltpu.VMEM((FF, WID), BF16),
            pltpu.VMEM((8, 32, TOK), F32),
            pltpu.VMEM((8 * TOK, WID), BF16),
            pltpu.VMEM((8 * TOK, WID), BF16),
            pltpu.VMEM((ROWS, WID), BF16),
            pltpu.VMEM((ROWS, WID), BF16),
            pltpu.VMEM((WID, ROWS), BF16),
            pltpu.VMEM((4, PAIR, WID), BF16),
            pltpu.VMEM((4, PAIR, WID), BF16),
            pltpu.VMEM((ROWS, 2 * FF), BF16),
            pltpu.VMEM((4, PAIR, 2 * FF), BF16),
            pltpu.VMEM((3, PAIR, 2 * FF), BF16),
            pltpu.VMEM((ROWS, FF), BF16),
            pltpu.VMEM((4, PAIR, FF), BF16),
            pltpu.VMEM((3, PAIR, FF), BF16),
            pltpu.VMEM((PAIR, 2 * FF), F32),
            pltpu.VMEM((ROWS, FF), BF16),
            pltpu.VMEM((ROWS, PU), BF16),
            pltpu.VMEM((ROWS, WID), BF16),
            pltpu.VMEM((4, PAIR, WID), BF16),
            pltpu.VMEM((ROWS, RW), BF16),
            pltpu.VMEM((4, PAIR, RW), BF16),
            pltpu.VMEM((4, 256, WID), BF16),
            pltpu.VMEM((4, 256, WID), BF16),
            pltpu.VMEM((8, WID, 256), BF16),
            pltpu.VMEM((8, WID, 256), BF16),
            pltpu.VMEM((4, 256, WID), BF16),
            pltpu.VMEM((8, WID, 256), BF16),
            pltpu.VMEM((8, TOK, WID), F32),
            pltpu.VMEM((8, TOK, RW), F32),
            pltpu.VMEM((8, TOK, WID), BF16),
            pltpu.VMEM((8, TOK, RW), BF16),
            pltpu.VMEM((8, TOK, WID), BF16),
            pltpu.VMEM((8, TOK, RW), BF16),
            pltpu.SemaphoreType.DMA((15,)),
            pltpu.SemaphoreType.DMA((N_SEM,)),
            pltpu.SemaphoreType.DMA((N_SEM,)),
        ],
        compiler_params=pltpu.CompilerParams(
            collective_id=0, has_side_effects=True, vmem_limit_bytes=67043328
        ),
    )(
        tokens,
        out_grad,
        route_lists.T,
        gate_values.T,
        expert_pairs.reshape(16, 1),
        gate_weight[0],
        up_weight[0],
        down_weight[0],
    )
    dots = sdot[:, 0:16] + sdot[:, 16:32]
    named = route_lists[:, :, None] == expert_pairs[None, None, :]
    gate_value_grad = jnp.sum(jnp.where(named, dots[:, None, :], 0.0), axis=2) / gate_values
    return out, grad, gate_value_grad, gg[None], gu[None], gd[None]


def solution(mesh):
    placed = (
        P("expert", "dp"),
        P("expert", "dp"),
        P("expert", None),
        P("expert", None),
        P(),
        P("expert", "dp", None),
        P("expert", "dp", None),
        P("expert", None, "dp"),
    )
    return jax.shard_map(
        shards,
        mesh=mesh,
        in_specs=placed,
        out_specs=(
            P("expert", "dp"),
            P("expert", "dp"),
            P("expert", None),
            P("expert", "dp", None),
            P("expert", "dp", None),
            P("expert", None, "dp"),
        ),
        check_vma=False,
    )
```
